16 devices in a mesh: dp: 2 (over y, z), cp: 8 (over x, core).
Axes of the slice: x: 4, y: 2, z: 1, core: 2. Of those that a mesh axis runs over, the one named last changes fastest.
The devices are a block of a 4x4x8 slice.
Arguments:
- x_tok: bfloat16 [12288, 5120], P(('dp', 'cp')), parts along dimension 0
- w_q: bfloat16 [5120, 5120], replicated
- w_k: bfloat16 [5120, 5120], replicated
- w_v: bfloat16 [5120, 5120], replicated
- w_o: bfloat16 [5120, 5120], replicated
Outputs:
- output 1: bfloat16 [12288, 5120], P(('dp', 'cp')), parts along dimension 0
- output 2: bfloat16 [12288, 40, 128], P(('dp', 'cp')), parts along dimension 0
- output 3: bfloat16 [12288, 40, 128], P(('dp', 'cp')), parts along dimension 0
There are 2 independent parts. The reference program is written for one: setup_inputs(seed, part) draws one part's arguments, and reference() takes and returns one part's arrays. A program takes and returns all parts, laid end to end along the dimension named above; an argument that names none is the same for every part.
All inputs are finite; a program needn't handle non-finite values.
Results may differ from the reference program's by a relative error of at most 0.00883212.
Values are sent between devices in bfloat16 or wider.
A program may use at most 768 MiB of HBM per device.

```python
import math
import jax
import jax.numpy as jnp
from jax import lax

D_MODEL = 5120
HEADS = 40
KV_HEADS = 40
HEAD = 128
TOKENS = 6144
CP_SIZE = 8
ROPE_BASE = 500000.0


def setup_inputs(seed: int = 0, part: int = 0) -> dict:
    part_key = jax.random.fold_in(jax.random.key(seed), part)
    w_keys = jax.random.split(jax.random.key(seed + 1), 4)
    x_tok = jax.random.normal(part_key, (TOKENS, D_MODEL), jnp.float32).astype(jnp.bfloat16)
    w_q = (jax.random.normal(w_keys[0], (D_MODEL, HEADS * HEAD), jnp.float32) * D_MODEL ** -0.5).astype(jnp.bfloat16)
    w_k = (jax.random.normal(w_keys[1], (D_MODEL, KV_HEADS * HEAD), jnp.float32) * D_MODEL ** -0.5).astype(jnp.bfloat16)
    w_v = (jax.random.normal(w_keys[2], (D_MODEL, KV_HEADS * HEAD), jnp.float32) * D_MODEL ** -0.5).astype(jnp.bfloat16)
    w_o = (jax.random.normal(w_keys[3], (HEADS * HEAD, D_MODEL), jnp.float32) * (HEADS * HEAD) ** -0.5).astype(jnp.bfloat16)
    return {'x_tok': x_tok, 'w_q': w_q, 'w_k': w_k, 'w_v': w_v, 'w_o': w_o}


def token_positions():
    rows = jnp.arange(TOKENS, dtype=jnp.int32)
    n_loc = TOKENS // CP_SIZE
    half_len = n_loc // 2
    dev_idx = rows // n_loc
    within = rows % n_loc
    piece = jnp.where(within < half_len, dev_idx, 2 * CP_SIZE - 1 - dev_idx)
    return piece * half_len + within % half_len


def rope_tables(tok_pos):
    inv_freq = 1.0 / (ROPE_BASE ** (jnp.arange(HEAD // 2, dtype=jnp.float32) * (2.0 / HEAD)))
    angles = tok_pos.astype(jnp.float32)[:, None] * inv_freq[None, :]
    return jnp.cos(angles)[:, None, :], jnp.sin(angles)[:, None, :]


def apply_rope(proj, rope_cos, rope_sin):
    first = proj[..., : HEAD // 2]
    second = proj[..., HEAD // 2:]
    return jnp.concatenate([first * rope_cos - second * rope_sin, second * rope_cos + first * rope_sin], axis=-1)


def reference(x_tok, w_q, w_k, w_v, w_o):
    tok_pos = token_positions()
    rope_cos, rope_sin = rope_tables(tok_pos)
    n_group = HEADS // KV_HEADS
    half_len = TOKENS // CP_SIZE // 2
    q_rot = apply_rope(jnp.dot(x_tok, w_q, preferred_element_type=jnp.float32).reshape(TOKENS, HEADS, HEAD), rope_cos, rope_sin).astype(jnp.bfloat16)
    k_rot = apply_rope(jnp.dot(x_tok, w_k, preferred_element_type=jnp.float32).reshape(TOKENS, KV_HEADS, HEAD), rope_cos, rope_sin).astype(jnp.bfloat16)
    v_val = jnp.dot(x_tok, w_v, preferred_element_type=jnp.float32).astype(jnp.bfloat16).reshape(TOKENS, KV_HEADS, HEAD)
    k_wide = k_rot.astype(jnp.float32)
    v_wide = v_val.astype(jnp.float32)
    q_blocks = q_rot.reshape(2 * CP_SIZE, half_len, KV_HEADS, n_group, HEAD)
    pos_blocks = tok_pos.reshape(2 * CP_SIZE, half_len)
    scale = 1.0 / math.sqrt(HEAD)

    def one_block(blk):
        q_blk, pos_blk = blk
        scores = jnp.einsum('nkgh,mkh->nkgm', q_blk.astype(jnp.float32), k_wide) * scale
        keep_mask = pos_blk[:, None] >= tok_pos[None, :]
        scores = jnp.where(keep_mask[:, None, None, :], scores, -jnp.inf)
        weights = jax.nn.softmax(scores, axis=-1)
        return jnp.einsum('nkgm,mkh->nkgh', weights, v_wide)

    attn_out = lax.map(one_block, (q_blocks, pos_blocks))
    attn_low = attn_out.reshape(TOKENS, HEADS * HEAD).astype(jnp.bfloat16)
    y_out = jnp.dot(attn_low, w_o, preferred_element_type=jnp.float32).astype(jnp.bfloat16)
    return (y_out, k_rot, v_val)
```

```python
import functools
import math

import jax
import jax.numpy as jnp
from jax import lax
from jax.experimental import pallas as pl
from jax.experimental.pallas import tpu as pltpu
from jax.sharding import PartitionSpec as P

HEAD = 128
ROPE_BASE = 500000.0
NEG_BIG = -1e30
EXP2_SCALE = math.log2(math.e) / math.sqrt(HEAD)
BQ = 1024
STREAM = 256
BK = 512


def rope_tables(tok_pos):
    inv_freq = 1.0 / (ROPE_BASE ** (jnp.arange(HEAD // 2, dtype=jnp.float32) * (2.0 / HEAD)))
    angles = tok_pos.astype(jnp.float32)[:, None] * inv_freq[None, :]
    cos, sin = jnp.cos(angles), jnp.sin(angles)
    return jnp.concatenate([cos, cos], axis=1), jnp.concatenate([-sin, sin], axis=1)


def local_positions(cp_rank, n_cp, half_len):
    offsets = jnp.arange(half_len, dtype=jnp.int32)
    return jnp.concatenate([cp_rank * half_len + offsets, (2 * n_cp - 1 - cp_rank) * half_len + offsets])


def project_kernel(n_chip, rank_ref, x_ref, wq_ref, wk_ref, wv_ref, cos_ref, sin_ref, kp_ref, vp_ref, *outs):
    step = pl.program_id(0)
    core = rank_ref[1]
    cos, sin = cos_ref[...], sin_ref[...]

    def emit(tensor, w_ref, plain_ref, rope):
        prod = jnp.dot(x_ref[...], w_ref[...], preferred_element_type=jnp.float32)
        heads = []
        for i in range(2):
            head = prod[:, i * HEAD:(i + 1) * HEAD]
            if rope:
                head = head * cos + pltpu.roll(head, HEAD // 2, 1) * sin
            heads.append(head)
        mine = jnp.where(core == 0, heads[0], heads[1]).astype(jnp.bfloat16)
        other = jnp.where(core == 0, heads[1], heads[0]).astype(jnp.bfloat16)
        if plain_ref is not None:
            for i in range(2):
                plain_ref[:, i * HEAD:(i + 1) * HEAD] = heads[i].astype(jnp.bfloat16)
        for d in range(n_chip):
            @pl.when(step == d)
            def _():
                outs[2 * d][tensor] = mine
                outs[2 * d + 1][tensor] = other

    emit(0, wq_ref, None, True)
    emit(1, wk_ref, kp_ref, True)
    emit(2, wv_ref, vp_ref, False)


def project(rank, x_loc, w_q, w_k, w_v, cos, sin, chunk, n_chip):
    n_loc, d_model = x_loc.shape
    width = 2 * HEAD

    def w_map(d, rank_ref):
        return 0, chunk * n_chip + lax.rem(rank_ref[0] + d, n_chip)

    def plain_map(d, rank_ref):
        return 0, lax.rem(rank_ref[0] + d, n_chip)

    whole = lambda d, rank_ref: (0, 0)
    w_spec = pl.BlockSpec((d_model, width), w_map)
    one = dict(pipeline_mode=pl.Buffered(1))
    piece = jax.ShapeDtypeStruct((3, n_loc, HEAD), jnp.bfloat16)
    plain = jax.ShapeDtypeStruct((n_loc, n_chip * width), jnp.bfloat16)
    return pl.pallas_call(
        functools.partial(project_kernel, n_chip),
        grid_spec=pltpu.PrefetchScalarGridSpec(
            num_scalar_prefetch=1,
            grid=(n_chip,),
            in_specs=[pl.BlockSpec((n_loc, d_model), whole, **one), w_spec, w_spec, w_spec,
                      pl.BlockSpec((n_loc, HEAD), whole, **one), pl.BlockSpec((n_loc, HEAD), whole, **one)],
            out_specs=[pl.BlockSpec((n_loc, width), plain_map)] * 2
            + [pl.BlockSpec((3, n_loc, HEAD), lambda d, rank_ref: (0, 0, 0), **one)] * (2 * n_chip),
        ),
        out_shape=[plain, plain] + [piece] * (2 * n_chip),
        compiler_params=pltpu.CompilerParams(dimension_semantics=("arbitrary",), vmem_limit_bytes=56 << 20),
        cost_estimate=pl.CostEstimate(flops=2 * n_loc * d_model * 3 * width * n_chip, bytes_accessed=3 * d_model * width * n_chip * 2, transcendentals=0),
        name=f"project{chunk}",
    )(rank, x_loc, w_q, w_k, w_v, cos, sin)


def attend_kernel(n_chip, half_len, rank_ref, *refs):
    n_src = 2 * n_chip
    srcs, outs = refs[:n_src], refs[n_src:2 * n_src]
    q_scr, k_scr, v_scr, vt_scr, o_scr, acc_scr, ml_scr, in_sem, out_sem = refs[2 * n_src:]
    chip, core = rank_ref[0], rank_ref[1]
    seq = q_scr.shape[0]
    n_pieces = 2 * n_src

    def owner(d, cross, sign):
        far = lax.rem(chip + (d if sign > 0 else n_chip - d), n_chip)
        return 2 * far + (1 - core if cross else core)

    def piece_rows(rank, half):
        index = rank if half == 0 else n_pieces - 1 - rank
        return pl.ds(pl.multiple_of(index * half_len, half_len), half_len)

    copies = []
    for d in range(n_chip):
        for cross in range(2):
            src = srcs[2 * d + cross]
            rank = owner(d, cross, -1)
            for half in range(2):
                for t, dst in enumerate((q_scr, k_scr, v_scr)):
                    copies.append(pltpu.make_async_copy(
                        src.at[t, pl.ds(half * half_len, half_len)], dst.at[piece_rows(rank, half)],
                        in_sem.at[2 * d + cross, half, t]))
    for copy in copies:
        copy.start()
    for copy in copies:
        copy.wait()

    @pl.loop(0, seq // BK)
    def _(i):
        rows = pl.ds(pl.multiple_of(i * BK, BK), BK)
        vt_scr[:, rows] = v_scr[rows, :].T

    n_stream = BQ // STREAM

    def update(u, q_u, k_rows, first, mask_off):
        k_blk = k_scr[k_rows, :]
        s = lax.dot_general(k_blk, q_u, (((1,), (1,)), ((), ())), preferred_element_type=jnp.float32)
        if mask_off is not None:
            key_at = lax.broadcasted_iota(jnp.int32, s.shape, 0)
            query_at = lax.broadcasted_iota(jnp.int32, s.shape, 1)
            s = jnp.where(key_at <= query_at + mask_off, s, NEG_BIG)
        cols = pl.ds(u * STREAM, STREAM)
        m_blk = jnp.max(s, axis=0, keepdims=True)
        if first:
            m_new = m_blk
        else:
            m_old = ml_scr[0:1, cols]
            m_new = jnp.maximum(m_old, m_blk)
        p = jnp.exp2(s * EXP2_SCALE - m_new * EXP2_SCALE)
        l_blk = jnp.sum(p, axis=0, keepdims=True)
        pv = jnp.dot(vt_scr[:, k_rows], p.astype(jnp.bfloat16), preferred_element_type=jnp.float32)
        if first:
            ml_scr[1:2, cols] = l_blk
            acc_scr[:, cols] = pv
        else:
            alpha = jnp.exp2((m_old - m_new) * EXP2_SCALE)
            ml_scr[1:2, cols] = ml_scr[1:2, cols] * alpha + l_blk
            acc_scr[:, cols] = acc_scr[:, cols] * alpha + pv
        ml_scr[0:1, cols] = m_new

    n_diag = BQ // BK

    @pl.loop(0, seq // BQ)
    def _(qi):
        q_base = pl.multiple_of(qi * BQ, BQ)
        q_u = [q_scr[pl.ds(q_base + u * STREAM, STREAM), :] for u in range(n_stream)]
        for b in range(n_diag):
            rows = pl.ds(pl.multiple_of(q_base + b * BK, BK), BK)
            for u in range(n_stream):
                off = u * STREAM - b * BK
                if off + STREAM - 1 < 0:
                    continue
                update(u, q_u[u], rows, b == 0, None if off >= BK - 1 else off)

        @pl.loop(0, qi * n_diag)
        def _(j):
            rows = pl.ds(pl.multiple_of(j * BK, BK), BK)
            for u in range(n_stream):
                update(u, q_u[u], rows, False, None)

        for u in range(n_stream):
            cols = pl.ds(u * STREAM, STREAM)
            out = acc_scr[:, cols] / ml_scr[1:2, cols]
            o_scr[pl.ds(q_base + u * STREAM, STREAM), :] = out.T.astype(jnp.bfloat16)

    copies = []
    for d in range(n_chip):
        for cross in range(2):
            rank = owner(d, cross, 1)
            for half in range(2):
                copies.append(pltpu.make_async_copy(
                    o_scr.at[piece_rows(rank, half)], outs[2 * d + cross].at[pl.ds(half * half_len, half_len)],
                    out_sem.at[2 * d + cross, half]))
    for copy in copies:
        copy.start()
    for copy in copies:
        copy.wait()


def attend(rank, pieces, n_chip, name):
    _, n_loc, _ = pieces[0].shape
    n_src = 2 * n_chip
    seq = n_loc * n_src
    hbm = pl.BlockSpec(memory_space=pltpu.HBM)
    flops = 2 * 2 * seq * seq * HEAD // 2
    return pl.pallas_call(
        functools.partial(attend_kernel, n_chip, n_loc // 2),
        in_specs=[pl.BlockSpec(memory_space=pltpu.SMEM)] + [hbm] * n_src,
        out_specs=[hbm] * n_src,
        out_shape=[jax.ShapeDtypeStruct((n_loc, HEAD), jnp.bfloat16)] * n_src,
        scratch_shapes=[pltpu.VMEM((seq, HEAD), jnp.bfloat16)] * 3
        + [pltpu.VMEM((HEAD, seq), jnp.bfloat16), pltpu.VMEM((seq, HEAD), jnp.bfloat16),
           pltpu.VMEM((HEAD, BQ), jnp.float32), pltpu.VMEM((8, BQ), jnp.float32),
           pltpu.SemaphoreType.DMA((n_src, 2, 3)), pltpu.SemaphoreType.DMA((n_src, 2))],
        compiler_params=pltpu.CompilerParams(vmem_limit_bytes=40 << 20),
        cost_estimate=pl.CostEstimate(flops=3 * flops, bytes_accessed=4 * seq * HEAD * 2, transcendentals=seq * seq // 2),
        name=name,
    )(rank, *pieces)


def combine_kernel(n_chip, n_chunk, has_prev, last, rank_ref, *refs):
    n_src = 2 * n_chip
    o_refs, refs = refs[:n_chunk * n_src], refs[n_chunk * n_src:]
    if has_prev:
        prev_ref, refs = refs[0], refs[1:]
    w_ref, y_ref, o_scr, sem = refs
    chip, core = rank_ref[0], rank_ref[1]

    @pl.when(pl.program_id(0) == 0)
    def _():
        copies = []
        for g in range(n_chunk):
            for d in range(n_chip):
                for cross in range(2):
                    head = 2 * lax.rem(chip + n_chip - d, n_chip) + (1 - core if cross else core)
                    cols = pl.ds(pl.multiple_of((g * n_src + head) * HEAD, HEAD), HEAD)
                    i = g * n_src + 2 * d + cross
                    copies.append(pltpu.make_async_copy(o_refs[i], o_scr.at[:, cols], sem.at[i]))
        for copy in copies:
            copy.start()
        for copy in copies:
            copy.wait()

    total = jnp.dot(o_scr[...], w_ref[...], preferred_element_type=jnp.float32)
    if has_prev:
        total = total + prev_ref[...]
    y_ref[...] = total.astype(y_ref.dtype)


def combine(rank, outs, prev, w_o, first_chunk, last, n_chip, name):
    n_chunk = len(outs)
    n_src = 2 * n_chip
    n_loc = outs[0][0].shape[0]
    depth, d_model = n_chunk * n_src * HEAD, w_o.shape[1]
    width = 512
    hbm = pl.BlockSpec(memory_space=pltpu.HBM)
    col = pl.BlockSpec((n_loc, width), lambda i: (0, i))
    lead = first_chunk * n_src * HEAD
    w_spec = pl.BlockSpec((pl.Element(depth), pl.Element(width)), lambda i: (lead, i * width))
    flat = [o for chunk in outs for o in chunk]
    return pl.pallas_call(
        functools.partial(combine_kernel, n_chip, n_chunk, prev is not None, last),
        grid=(d_model // width,),
        in_specs=[pl.BlockSpec(memory_space=pltpu.SMEM)] + [hbm] * len(flat) + ([col] if prev is not None else []) + [w_spec],
        out_specs=col,
        out_shape=jax.ShapeDtypeStruct((n_loc, d_model), jnp.bfloat16 if last else jnp.float32),
        scratch_shapes=[pltpu.VMEM((n_loc, depth), jnp.bfloat16), pltpu.SemaphoreType.DMA((len(flat),))],
        compiler_params=pltpu.CompilerParams(dimension_semantics=("arbitrary",), vmem_limit_bytes=48 << 20),
        cost_estimate=pl.CostEstimate(flops=2 * n_loc * depth * d_model, bytes_accessed=depth * d_model * 2, transcendentals=0),
        name=name,
    )(rank, *flat, *([prev] if prev is not None else []), w_o)


def solution(mesh):
    n_cp = mesh.shape['cp']
    n_chip = n_cp // 2

    def shift(d, cross):
        return [(2 * c + k, 2 * ((c + d) % n_chip) + (1 - k if cross else k)) for c in range(n_chip) for k in range(2)]

    def exchange(pieces):
        got = []
        for d in range(n_chip):
            for cross in range(2):
                piece = pieces[2 * d + cross]
                got.append(lax.ppermute(piece, 'cp', shift(d, cross)) if d or cross else piece)
        return got

    def per_device(x_loc, w_q, w_k, w_v, w_o):
        n_loc = x_loc.shape[0]
        n_heads = w_q.shape[1] // HEAD
        n_chunk = n_heads // n_cp
        cp_rank = lax.axis_index('cp')
        rank = jnp.stack([cp_rank // 2, cp_rank % 2]).astype(jnp.int32)
        cos, sin = rope_tables(local_positions(cp_rank, n_cp, n_loc // 2))
        k_parts, v_parts, outs = [], [], []
        for g in range(n_chunk):
            k_plain, v_plain, *pieces = project(rank, x_loc, w_q, w_k, w_v, cos, sin, g, n_chip)
            k_parts.append(k_plain.reshape(n_loc, n_cp, HEAD))
            v_parts.append(v_plain.reshape(n_loc, n_cp, HEAD))
            outs.append(exchange(attend(rank, exchange(pieces), n_chip, f"attend{g}")))
        part = combine(rank, outs[:-1], None, w_o, 0, False, n_chip, "combine_head")
        y_loc = combine(rank, outs[-1:], part, w_o, n_chunk - 1, True, n_chip, "combine_tail")
        return y_loc, jnp.concatenate(k_parts, axis=1), jnp.concatenate(v_parts, axis=1)

    row_spec = P(('dp', 'cp'), None)
    kv_spec = P(('dp', 'cp'), None, None)
    full_spec = P(None, None)
    return jax.shard_map(per_device, mesh=mesh, in_specs=(row_spec, full_spec, full_spec, full_spec, full_spec), out_specs=(row_spec, kv_spec, kv_spec), check_vma=False)
```

```python
import functools
import math

import jax
import jax.numpy as jnp
from jax import lax
from jax.experimental import pallas as pl
from jax.experimental.pallas import tpu as pltpu
from jax.sharding import PartitionSpec as P

HEAD = 128
ROPE_BASE = 500000.0
NEG_BIG = -1e30
EXP2_SCALE = math.log2(math.e) / math.sqrt(HEAD)
BQ = 1024
STREAM = 256
BK = 512
ROW_STEP = 256
LANES = 2 * HEAD
OUT_COLS = 512
MESH = pl.DeviceIdType.MESH


def rope_tables(tok_pos):
    inv_freq = 1.0 / (ROPE_BASE ** (jnp.arange(HEAD // 2, dtype=jnp.float32) * (2.0 / HEAD)))
    angles = tok_pos.astype(jnp.float32)[:, None] * inv_freq[None, :]
    cos, sin = jnp.cos(angles), jnp.sin(angles)
    return jnp.concatenate([cos, cos], axis=1), jnp.concatenate([-sin, sin], axis=1)


def local_positions(cp_rank, n_cp, half_len):
    offsets = jnp.arange(half_len, dtype=jnp.int32)
    return jnp.concatenate([cp_rank * half_len + offsets, (2 * n_cp - 1 - cp_rank) * half_len + offsets])


def layer_kernel(n_cp, n_chunk, x_hbm, wq_hbm, wk_hbm, wv_hbm, wo_hbm, cos_ref, sin_ref,
                 y_hbm, kp_hbm, vp_hbm, send_hbm, got_hbm, ogot_hbm,
                 x_scr, w_scr, h_scr, q_scr, k_scr, v_scr, vt_scr, o_scr, acc_scr, ml_scr, mx_scr, s0_scr, s1_scr,
                 oc_scr, wo_scr, y_scr, ys_scr,
                 x_sem, w_sem, h_sem, send_sem, recv_sem, in_sem, oself_sem, osend_sem, orecv_sem, oc_sem, wo_sem, ys_sem):
    me = lax.axis_index('cp')
    n_chip = n_cp // 2
    chip = lax.div(me, 2)
    n_loc = x_scr.shape[0]
    half_len = n_loc // 2
    seq = n_loc * n_cp
    n_pieces = 2 * n_cp
    n_stream = BQ // STREAM
    n_out = y_scr.shape[1] // OUT_COLS
    depth = n_cp * HEAD

    barrier = pltpu.get_barrier_semaphore()
    for other in range(n_cp):
        @pl.when(me != other)
        def _():
            pl.semaphore_signal(barrier, inc=1, device_id={'cp': other}, device_id_type=MESH)
    pl.semaphore_wait(barrier, n_cp - 1)

    def dest_chip(step):
        return lax.rem(chip + step + 1, n_chip)

    def w_copy(g, step, t):
        col = pl.multiple_of((g * n_chip + dest_chip(step)) * LANES, LANES)
        return pltpu.make_async_copy((wq_hbm, wk_hbm, wv_hbm)[t].at[:, pl.ds(col, LANES)], w_scr.at[t], w_sem.at[t])

    x_copy = pltpu.make_async_copy(x_hbm, x_scr, x_sem)
    x_copy.start()
    for t in range(3):
        w_copy(0, 0, t).start()
    y_scr[...] = jnp.zeros_like(y_scr)
    x_copy.wait()

    def to_peer(g, dest):
        return pltpu.make_async_remote_copy(
            src_ref=send_hbm.at[g, dest], dst_ref=got_hbm.at[g, me], send_sem=send_sem.at[g, dest],
            recv_sem=recv_sem.at[g, me], device_id={'cp': dest}, device_id_type=MESH)

    def from_peer(g, src):
        return pltpu.make_async_remote_copy(
            src_ref=send_hbm.at[g, src], dst_ref=got_hbm.at[g, src], send_sem=send_sem.at[g, src],
            recv_sem=recv_sem.at[g, src], device_id={'cp': src}, device_id_type=MESH)

    def spill(g, step, i):
        par = lax.rem(step, 2)
        dest = 2 * dest_chip(step) + i
        col = pl.ds(pl.multiple_of((g * n_cp + dest) * HEAD, HEAD), HEAD)
        mine = pltpu.make_async_copy(h_scr.at[par, i], got_hbm.at[g, dest], h_sem.at[par, i, 0])
        other = pltpu.make_async_copy(h_scr.at[par, i], send_hbm.at[g, dest], h_sem.at[par, i, 0])
        plain = [pltpu.make_async_copy(h_scr.at[par, i, 1], kp_hbm.at[:, col], h_sem.at[par, i, 1]),
                 pltpu.make_async_copy(h_scr.at[par, i, 2], vp_hbm.at[:, col], h_sem.at[par, i, 2])]
        return dest, mine, other, plain

    def spill_start(g, step):
        for i in range(2):
            dest, mine, other, plain = spill(g, step, i)

            @pl.when(dest == me)
            def _():
                mine.start()

            @pl.when(dest != me)
            def _():
                other.start()
            for copy in plain:
                copy.start()

    def spill_send(g, step):
        for i in range(2):
            dest, mine, other, plain = spill(g, step, i)

            @pl.when(dest == me)
            def _():
                mine.wait()

            @pl.when(dest != me)
            def _():
                other.wait()
                to_peer(g, dest).start()
            for copy in plain:
                copy.wait()

    def project(g):
        @pl.loop(0, n_chip)
        def _(step):
            par = lax.rem(step, 2)
            for t in range(3):
                w_copy(g, step, t).wait()
                prod = jnp.dot(x_scr[...], w_scr[t], preferred_element_type=jnp.float32)
                for i in range(2):
                    head = prod[:, i * HEAD:(i + 1) * HEAD]
                    if t < 2:
                        head = head * cos_ref[...] + pltpu.roll(head, HEAD // 2, 1) * sin_ref[...]
                    h_scr[par, i, t] = head.astype(jnp.bfloat16)
                later = g * n_chip + step + 1

                @pl.when(later < n_chunk * n_chip)
                def _():
                    w_copy(lax.div(later, n_chip), lax.rem(later, n_chip), t).start()
                if t == 0:
                    @pl.when(step > 0)
                    def _():
                        spill_send(g, step - 1)
            spill_start(g, step)
        spill_send(g, n_chip - 1)

    def home(piece):
        return (piece, 0) if piece < n_cp else (n_pieces - 1 - piece, 1)

    def rows_of(piece):
        return pl.ds(piece * half_len, half_len)

    def load(g, piece):
        src, half = home(piece)
        return [pltpu.make_async_copy(got_hbm.at[g, src, t, pl.ds(half * half_len, half_len)], dst.at[rows_of(piece)], in_sem.at[piece, t])
                for t, dst in enumerate((q_scr, k_scr, v_scr))]

    def o_send(g, piece):
        dest, half = home(piece)
        par = lax.rem(g, 2)
        return pltpu.make_async_remote_copy(
            src_ref=o_scr.at[par, rows_of(piece)], dst_ref=ogot_hbm.at[g, me, pl.ds(half * half_len, half_len)],
            send_sem=osend_sem.at[par, piece], recv_sem=orecv_sem.at[g, me, half], device_id={'cp': dest}, device_id_type=MESH)

    def o_keep(g, piece):
        dest, half = home(piece)
        return pltpu.make_async_copy(o_scr.at[lax.rem(g, 2), rows_of(piece)], ogot_hbm.at[g, dest, pl.ds(half * half_len, half_len)], oself_sem.at[half])

    def o_recv(g, src, half):
        return pltpu.make_async_remote_copy(
            src_ref=o_scr.at[0, pl.ds(0, half_len)], dst_ref=ogot_hbm.at[g, src, pl.ds(half * half_len, half_len)],
            send_sem=osend_sem.at[0, 0], recv_sem=orecv_sem.at[g, src, half], device_id={'cp': src}, device_id_type=MESH)

    def o_sent(g):
        for piece in range(n_pieces):
            @pl.when(home(piece)[0] != me)
            def _():
                o_send(g, piece).wait_send()

    def scores(u, q_u, k_base, s_scr, slot, off):
        cols = slice(u * STREAM, (u + 1) * STREAM)
        top = None
        for r in range(0, BK, ROW_STEP):
            k_blk = k_scr[pl.ds(k_base + r, ROW_STEP), :]
            s = lax.dot_general(k_blk, q_u, (((1,), (1,)), ((), ())), preferred_element_type=jnp.float32)
            if off is not None and off - r < ROW_STEP - 1:
                key_at = lax.broadcasted_iota(jnp.int32, s.shape, 0)
                query_at = lax.broadcasted_iota(jnp.int32, s.shape, 1)
                s = jnp.where(key_at <= query_at + (off - r), s, NEG_BIG)
            s_scr[r:r + ROW_STEP, cols] = s
            blk_top = jnp.max(s, axis=0, keepdims=True)
            top = blk_top if top is None else jnp.maximum(top, blk_top)
        mx_scr[slot:slot + 1, cols] = top

    def fold(u, k_base, s_scr, slot, first):
        cols = slice(u * STREAM, (u + 1) * STREAM)
        m_new = mx_scr[slot:slot + 1, cols]
        if not first:
            m_old = ml_scr[0:1, cols]
            m_new = jnp.maximum(m_old, m_new)
        shift = m_new * EXP2_SCALE
        p = jnp.exp2(s_scr[:, cols] * EXP2_SCALE - shift)
        l_blk = jnp.sum(p, axis=0, keepdims=True)
        pv = jnp.dot(vt_scr[:, pl.ds(k_base, BK)], p.astype(jnp.bfloat16), preferred_element_type=jnp.float32)
        if first:
            ml_scr[1:2, cols] = l_blk
            acc_scr[:, cols] = pv
        else:
            alpha = jnp.exp2(m_old * EXP2_SCALE - shift)
            ml_scr[1:2, cols] = ml_scr[1:2, cols] * alpha + l_blk
            acc_scr[:, cols] = acc_scr[:, cols] * alpha + pv
        ml_scr[0:1, cols] = m_new

    def diag_off(u, b):
        off = u * STREAM - b * BK
        return None if off >= BK - 1 else off

    def attend(g):
        @pl.when(g >= 2)
        def _():
            o_sent(g - 2)
        for src in range(n_cp):
            @pl.when(me != src)
            def _():
                from_peer(g, src).wait_recv()
        for piece in range(n_pieces):
            for copy in load(g, piece):
                copy.start()
        par = lax.rem(g, 2)

        @pl.loop(0, seq // BQ)
        def _(qi):
            q_base = pl.multiple_of(qi * BQ, BQ)
            for i in range(seq // BQ):
                @pl.when(qi == i)
                def _():
                    for piece in range(-(-i * BQ // half_len), -(-(i + 1) * BQ // half_len)):
                        for copy in load(g, piece):
                            copy.wait()

            for r in range(0, BQ, BK):
                rows = pl.ds(pl.multiple_of(q_base + r, BK), BK)
                vt_scr[:, rows] = v_scr[rows, :].T
            q_u = [q_scr[pl.ds(q_base + u * STREAM, STREAM), :] for u in range(n_stream)]
            diag0, diag1 = q_base, pl.multiple_of(q_base + BK, BK)
            for u in range(n_stream):
                scores(u, q_u[u], diag0, s0_scr, 0, diag_off(u, 0))
            for u in range(n_stream):
                if (u + 1) * STREAM > BK:
                    scores(u, q_u[u], diag1, s1_scr, 1, diag_off(u, 1))
                fold(u, diag0, s0_scr, 0, True)
            for u in range(n_stream):
                scores(u, q_u[u], 0, s0_scr, 0, None)
                if (u + 1) * STREAM > BK:
                    fold(u, diag1, s1_scr, 1, False)

            @pl.loop(0, qi)
            def _(t):
                blk0 = pl.multiple_of(t * (2 * BK), 2 * BK)
                blk1, blk2 = pl.multiple_of(blk0 + BK, BK), pl.multiple_of(blk0 + 2 * BK, BK)
                for u in range(n_stream):
                    scores(u, q_u[u], blk1, s1_scr, 1, None)
                    fold(u, blk0, s0_scr, 0, False)
                for u in range(n_stream):
                    scores(u, q_u[u], blk2, s0_scr, 0, None)
                    fold(u, blk1, s1_scr, 1, False)

            for u in range(n_stream):
                cols = slice(u * STREAM, (u + 1) * STREAM)
                out = acc_scr[:, cols] / ml_scr[1:2, cols]
                o_scr[par, pl.ds(q_base + u * STREAM, STREAM), :] = out.T.astype(jnp.bfloat16)
            for i in range(seq // BQ):
                @pl.when(qi == i)
                def _():
                    for piece in range(i * BQ // half_len, (i + 1) * BQ // half_len):
                        @pl.when(home(piece)[0] == me)
                        def _():
                            o_keep(g, piece).start()

                        @pl.when(home(piece)[0] != me)
                        def _():
                            o_send(g, piece).start()
        for piece in range(n_pieces):
            @pl.when(home(piece)[0] == me)
            def _():
                o_keep(g, piece).wait()

    def wo_copy(g, nb, slot):
        rows = pl.ds(pl.multiple_of(g * depth, depth), depth)
        return pltpu.make_async_copy(wo_hbm.at[rows, pl.ds(pl.multiple_of(nb * OUT_COLS, OUT_COLS), OUT_COLS)], wo_scr.at[slot], wo_sem.at[slot])

    def y_copy(nb, slot):
        return pltpu.make_async_copy(ys_scr.at[slot], y_hbm.at[:, pl.ds(pl.multiple_of(nb * OUT_COLS, OUT_COLS), OUT_COLS)], ys_sem.at[slot])

    def combine(g):
        wo_copy(g, 0, 0).start()
        wo_copy(g, 1, 1).start()
        for src in range(n_cp):
            @pl.when(me != src)
            def _():
                for half in range(2):
                    o_recv(g, src, half).wait_recv()
        loads = [pltpu.make_async_copy(ogot_hbm.at[g, h], oc_scr.at[:, pl.ds(h * HEAD, HEAD)], oc_sem.at[h]) for h in range(n_cp)]
        for copy in loads:
            copy.start()
        for copy in loads:
            copy.wait()

        @pl.loop(0, n_out)
        def _(nb):
            slot = lax.rem(nb, 2)
            cols = pl.ds(pl.multiple_of(nb * OUT_COLS, OUT_COLS), OUT_COLS)
            wo_copy(g, nb, slot).wait()
            y_scr[:, cols] += jnp.dot(oc_scr[...], wo_scr[slot], preferred_element_type=jnp.float32)

            @pl.when(nb + 2 < n_out)
            def _():
                wo_copy(g, nb + 2, slot).start()

            @pl.when(g == n_chunk - 1)
            def _():
                @pl.when(nb >= 2)
                def _():
                    y_copy(nb - 2, slot).wait()
                ys_scr[slot] = y_scr[:, cols].astype(jnp.bfloat16)
                y_copy(nb, slot).start()

    @pl.loop(0, n_chunk + 4)
    def _(i):
        @pl.when(i < n_chunk)
        def _():
            project(i)

        @pl.when(jnp.logical_and(i >= 2, i < n_chunk + 2))
        def _():
            attend(i - 2)

        @pl.when(i >= 4)
        def _():
            combine(i - 4)

    for nb in range(n_out - 2, n_out):
        y_copy(nb, nb % 2).wait()
    for g in range(max(n_chunk - 2, 0), n_chunk):
        o_sent(g)

    @pl.loop(0, n_chunk)
    def _(g):
        for dest in range(n_cp):
            @pl.when(me != dest)
            def _():
                to_peer(g, dest).wait_send()


def layer(x_loc, w_q, w_k, w_v, w_o, cos, sin, n_cp):
    n_loc, d_model = x_loc.shape
    width = w_q.shape[1]
    n_chunk = width // HEAD // n_cp
    seq = n_loc * n_cp
    bf16, f32 = jnp.bfloat16, jnp.float32
    shape = jax.ShapeDtypeStruct
    hbm = pl.BlockSpec(memory_space=pltpu.HBM)
    vmem = pl.BlockSpec(memory_space=pltpu.VMEM)
    dma = pltpu.SemaphoreType.DMA
    rows = pltpu.VMEM((seq, HEAD), bf16)
    stats = pltpu.VMEM((8, BQ), f32)
    score = pltpu.VMEM((BK, BQ), f32)
    pieces = shape((n_chunk, n_cp, 3, n_loc, HEAD), bf16)
    y, k_plain, v_plain, *_ = pl.pallas_call(
        functools.partial(layer_kernel, n_cp, n_chunk),
        in_specs=[hbm] * 5 + [vmem] * 2,
        out_specs=[hbm] * 6,
        out_shape=[shape((n_loc, w_o.shape[1]), bf16), shape((n_loc, width), bf16), shape((n_loc, width), bf16),
                   pieces, pieces, shape((n_chunk, n_cp, n_loc, HEAD), bf16)],
        scratch_shapes=[
            pltpu.VMEM((n_loc, d_model), bf16), pltpu.VMEM((3, d_model, LANES), bf16), pltpu.VMEM((2, 2, 3, n_loc, HEAD), bf16),
            rows, rows, rows, pltpu.VMEM((HEAD, seq), bf16), pltpu.VMEM((2, seq, HEAD), bf16), pltpu.VMEM((HEAD, BQ), f32),
            stats, stats, score, score,
            pltpu.VMEM((n_loc, n_cp * HEAD), bf16), pltpu.VMEM((2, n_cp * HEAD, OUT_COLS), bf16), pltpu.VMEM((n_loc, w_o.shape[1]), f32),
            pltpu.VMEM((2, n_loc, OUT_COLS), bf16),
            dma, dma((3,)), dma((2, 2, 3)), dma((n_chunk, n_cp)), dma((n_chunk, n_cp)), dma((2 * n_cp, 3)), dma((2,)),
            dma((2, 2 * n_cp)), dma((n_chunk, n_cp, 2)), dma((n_cp,)), dma((2,)), dma((2,))],
        compiler_params=pltpu.CompilerParams(collective_id=0, has_side_effects=True, vmem_limit_bytes=62 << 20),
        name="layer",
    )(x_loc, w_q, w_k, w_v, w_o, cos, sin)
    return y, k_plain, v_plain


def solution(mesh):
    n_cp = mesh.shape['cp']

    def per_device(x_loc, w_q, w_k, w_v, w_o):
        n_loc = x_loc.shape[0]
        cos, sin = rope_tables(local_positions(lax.axis_index('cp'), n_cp, n_loc // 2))
        y_loc, k_plain, v_plain = layer(x_loc, w_q, w_k, w_v, w_o, cos, sin, n_cp)
        return y_loc, k_plain.reshape(n_loc, -1, HEAD), v_plain.reshape(n_loc, -1, HEAD)

    row_spec = P(('dp', 'cp'), None)
    kv_spec = P(('dp', 'cp'), None, None)
    full_spec = P(None, None)
    return jax.shard_map(per_device, mesh=mesh, in_specs=(row_spec, full_spec, full_spec, full_spec, full_spec), out_specs=(row_spec, kv_spec, kv_spec), check_vma=False)
```

```python
import functools
import math

import jax
import jax.numpy as jnp
from jax import lax
from jax.experimental import pallas as pl
from jax.experimental.pallas import tpu as pltpu
from jax.sharding import PartitionSpec as P

HEAD = 128
ROPE_BASE = 500000.0
NEG_BIG = -1e30
EXP2_SCALE = math.log2(math.e) / math.sqrt(HEAD)
BQ = 1024
STREAM = 256
BK = 512
ROW_STEP = 256
LANES = 2 * HEAD
OUT_COLS = 1024
COPY_ROWS = 128
MESH = pl.DeviceIdType.MESH


def rope_tables(tok_pos):
    lane = jnp.arange(HEAD, dtype=jnp.int32)
    inv_freq = 1.0 / (ROPE_BASE ** ((lane % (HEAD // 2)).astype(jnp.float32) * (2.0 / HEAD)))
    angles = tok_pos.astype(jnp.float32)[:, None] * inv_freq[None, :]
    sin = jnp.sin(angles)
    return jnp.cos(angles), jnp.where(lane[None, :] < HEAD // 2, -sin, sin)


def local_positions(cp_rank, n_cp, half_len):
    offsets = jnp.arange(half_len, dtype=jnp.int32)
    return jnp.concatenate([cp_rank * half_len + offsets, (2 * n_cp - 1 - cp_rank) * half_len + offsets])


def layer_kernel(n_cp, n_chunk, x_hbm, wq_hbm, wk_hbm, wv_hbm, wo_hbm, cos_ref, sin_ref,
                 y_hbm, kp_hbm, vp_hbm, send_hbm, got_hbm, ogot_hbm,
                 x_scr, w_scr, h_scr, q_scr, k_scr, v_scr, vt_scr, o_scr, acc_scr, ml_scr, mx_scr, s0_scr, s1_scr,
                 oc_scr, wo_scr, y_scr, ys_scr,
                 x_sem, w_sem, h_sem, send_sem, recv_sem, in_sem, oself_sem, osend_sem, orecv_sem, oc_sem, wo_sem, ys_sem):
    me = lax.axis_index('cp')
    n_chip = n_cp // 2
    chip = lax.div(me, 2)
    n_loc = x_scr.shape[0]
    half_len = n_loc // 2
    seq = n_loc * n_cp
    n_pieces = 2 * n_cp
    n_stream = BQ // STREAM
    n_out = y_scr.shape[1] // OUT_COLS
    depth = n_cp * HEAD
    row_parts = [slice(r, r + half_len) for r in range(0, n_loc, half_len)]

    barrier = pltpu.get_barrier_semaphore()
    for other in range(n_cp):
        @pl.when(me != other)
        def _():
            pl.semaphore_signal(barrier, inc=1, device_id={'cp': other}, device_id_type=MESH)
    pl.semaphore_wait(barrier, n_cp - 1)

    def dest_chip(step):
        return lax.rem(chip + step + 1, n_chip)

    def w_copy(g, step, t):
        col = pl.multiple_of((g * n_chip + dest_chip(step)) * LANES, LANES)
        return pltpu.make_async_copy((wq_hbm, wk_hbm, wv_hbm)[t].at[:, pl.ds(col, LANES)], w_scr.at[t], w_sem.at[t])

    x_copy = pltpu.make_async_copy(x_hbm, x_scr, x_sem)
    x_copy.start()
    for t in range(3):
        w_copy(0, 0, t).start()
    y_scr[...] = jnp.zeros_like(y_scr)
    x_copy.wait()

    def to_peer(g, dest):
        return pltpu.make_async_remote_copy(
            src_ref=send_hbm.at[g, dest], dst_ref=got_hbm.at[g, me], send_sem=send_sem.at[g, dest],
            recv_sem=recv_sem.at[g, me], device_id={'cp': dest}, device_id_type=MESH)

    def from_peer(g, src):
        return pltpu.make_async_remote_copy(
            src_ref=send_hbm.at[g, src], dst_ref=got_hbm.at[g, src], send_sem=send_sem.at[g, src],
            recv_sem=recv_sem.at[g, src], device_id={'cp': src}, device_id_type=MESH)

    def spill(g, step, i):
        par = lax.rem(step, 2)
        dest = 2 * dest_chip(step) + i
        col = pl.ds(pl.multiple_of((g * n_cp + dest) * HEAD, HEAD), HEAD)
        mine = pltpu.make_async_copy(h_scr.at[par, i], got_hbm.at[g, dest], h_sem.at[par, i, 0])
        other = pltpu.make_async_copy(h_scr.at[par, i], send_hbm.at[g, dest], h_sem.at[par, i, 0])
        plain = [pltpu.make_async_copy(h_scr.at[par, i, 1], kp_hbm.at[:, col], h_sem.at[par, i, 1]),
                 pltpu.make_async_copy(h_scr.at[par, i, 2], vp_hbm.at[:, col], h_sem.at[par, i, 2])]
        return dest, mine, other, plain

    def spill_start(g, step):
        for i in range(2):
            dest, mine, other, plain = spill(g, step, i)

            @pl.when(dest == me)
            def _():
                mine.start()

            @pl.when(dest != me)
            def _():
                other.start()
            for copy in plain:
                copy.start()

    def spill_send(g, step):
        for i in range(2):
            dest, mine, other, plain = spill(g, step, i)

            @pl.when(dest == me)
            def _():
                mine.wait()

            @pl.when(dest != me)
            def _():
                other.wait()
                to_peer(g, dest).start()
            for copy in plain:
                copy.wait()

    def project(g):
        @pl.loop(0, n_chip)
        def _(step):
            par = lax.rem(step, 2)
            for t in range(3):
                w_copy(g, step, t).wait()
                for rows in row_parts:
                    prod = jnp.dot(x_scr[rows, :], w_scr[t], preferred_element_type=jnp.float32)
                    for i in range(2):
                        head = prod[:, i * HEAD:(i + 1) * HEAD]
                        if t < 2:
                            head = head * cos_ref[rows, :] + pltpu.roll(head, HEAD // 2, 1) * sin_ref[rows, :]
                        h_scr[par, i, t, rows] = head.astype(jnp.bfloat16)
                later = g * n_chip + step + 1

                @pl.when(later < n_chunk * n_chip)
                def _():
                    w_copy(lax.div(later, n_chip), lax.rem(later, n_chip), t).start()
                if t == 0:
                    @pl.when(step > 0)
                    def _():
                        spill_send(g, step - 1)
            spill_start(g, step)
        spill_send(g, n_chip - 1)

    def home(piece):
        return (piece, 0) if piece < n_cp else (n_pieces - 1 - piece, 1)

    def rows_of(piece):
        return pl.ds(piece * half_len, half_len)

    def load(g, piece):
        src, half = home(piece)
        return [pltpu.make_async_copy(got_hbm.at[g, src, t, pl.ds(half * half_len, half_len)], dst.at[rows_of(piece)], in_sem.at[piece, t])
                for t, dst in enumerate((q_scr, k_scr, v_scr))]

    def o_send(g, piece):
        dest, half = home(piece)
        return pltpu.make_async_remote_copy(
            src_ref=o_scr.at[g, rows_of(piece)], dst_ref=ogot_hbm.at[g, me, pl.ds(half * half_len, half_len)],
            send_sem=osend_sem.at[g, piece], recv_sem=orecv_sem.at[g, me, half], device_id={'cp': dest}, device_id_type=MESH)

    def o_keep(g, piece):
        dest, half = home(piece)
        return pltpu.make_async_copy(o_scr.at[g, rows_of(piece)], ogot_hbm.at[g, dest, pl.ds(half * half_len, half_len)], oself_sem.at[half])

    def o_recv(g, src, half):
        return pltpu.make_async_remote_copy(
            src_ref=o_scr.at[0, pl.ds(0, half_len)], dst_ref=ogot_hbm.at[g, src, pl.ds(half * half_len, half_len)],
            send_sem=osend_sem.at[0, 0], recv_sem=orecv_sem.at[g, src, half], device_id={'cp': src}, device_id_type=MESH)

    def o_sent(g):
        for piece in range(n_pieces):
            @pl.when(home(piece)[0] != me)
            def _():
                o_send(g, piece).wait_send()

    def scores(u, q_u, k_base, s_scr, slot, off):
        cols = slice(u * STREAM, (u + 1) * STREAM)
        top = None
        for r in range(0, BK, ROW_STEP):
            k_blk = k_scr[pl.ds(k_base + r, ROW_STEP), :]
            s = lax.dot_general(k_blk, q_u, (((1,), (1,)), ((), ())), preferred_element_type=jnp.float32)
            if off is not None and off - r < ROW_STEP - 1:
                key_at = lax.broadcasted_iota(jnp.int32, s.shape, 0)
                query_at = lax.broadcasted_iota(jnp.int32, s.shape, 1)
                s = jnp.where(key_at <= query_at + (off - r), s, NEG_BIG)
            s_scr[r:r + ROW_STEP, cols] = s
            blk_top = jnp.max(s, axis=0, keepdims=True)
            top = blk_top if top is None else jnp.maximum(top, blk_top)
        mx_scr[slot:slot + 1, cols] = top

    def fold(u, k_base, s_scr, slot, first):
        cols = slice(u * STREAM, (u + 1) * STREAM)
        m_new = mx_scr[slot:slot + 1, cols]
        if not first:
            m_old = ml_scr[0:1, cols]
            m_new = jnp.maximum(m_old, m_new)
        shift = m_new * EXP2_SCALE
        p = jnp.exp2(s_scr[:, cols] * EXP2_SCALE - shift)
        l_blk = jnp.sum(p, axis=0, keepdims=True)
        pv = jnp.dot(vt_scr[:, pl.ds(k_base, BK)], p.astype(jnp.bfloat16), preferred_element_type=jnp.float32)
        if first:
            ml_scr[1:2, cols] = l_blk
            acc_scr[:, cols] = pv
        else:
            alpha = jnp.exp2(m_old * EXP2_SCALE - shift)
            ml_scr[1:2, cols] = ml_scr[1:2, cols] * alpha + l_blk
            acc_scr[:, cols] = acc_scr[:, cols] * alpha + pv
        ml_scr[0:1, cols] = m_new

    def diag_off(u, b):
        off = u * STREAM - b * BK
        return None if off >= BK - 1 else off

    def attend(g):
        for src in range(n_cp):
            @pl.when(me != src)
            def _():
                from_peer(g, src).wait_recv()
        for piece in range(n_pieces):
            for copy in load(g, piece):
                copy.start()

        @pl.loop(0, seq // BQ)
        def _(qi):
            q_base = pl.multiple_of(qi * BQ, BQ)
            for i in range(seq // BQ):
                @pl.when(qi == i)
                def _():
                    for piece in range(-(-i * BQ // half_len), -(-(i + 1) * BQ // half_len)):
                        for copy in load(g, piece):
                            copy.wait()

            for r in range(0, BQ, BK):
                rows = pl.ds(pl.multiple_of(q_base + r, BK), BK)
                vt_scr[:, rows] = v_scr[rows, :].T
            q_u = [q_scr[pl.ds(q_base + u * STREAM, STREAM), :] for u in range(n_stream)]
            diag0, diag1 = q_base, pl.multiple_of(q_base + BK, BK)
            for u in range(n_stream):
                scores(u, q_u[u], diag0, s0_scr, 0, diag_off(u, 0))
            for u in range(n_stream):
                if (u + 1) * STREAM > BK:
                    scores(u, q_u[u], diag1, s1_scr, 1, diag_off(u, 1))
                fold(u, diag0, s0_scr, 0, True)
            for u in range(n_stream):
                scores(u, q_u[u], 0, s0_scr, 0, None)
                if (u + 1) * STREAM > BK:
                    fold(u, diag1, s1_scr, 1, False)

            @pl.loop(0, qi)
            def _(t):
                blk0 = pl.multiple_of(t * (2 * BK), 2 * BK)
                blk1, blk2 = pl.multiple_of(blk0 + BK, BK), pl.multiple_of(blk0 + 2 * BK, BK)
                for u in range(n_stream):
                    scores(u, q_u[u], blk1, s1_scr, 1, None)
                    fold(u, blk0, s0_scr, 0, False)
                for u in range(n_stream):
                    scores(u, q_u[u], blk2, s0_scr, 0, None)
                    fold(u, blk1, s1_scr, 1, False)

            for u in range(n_stream):
                cols = slice(u * STREAM, (u + 1) * STREAM)
                out = acc_scr[:, cols] / ml_scr[1:2, cols]
                o_scr[g, pl.ds(q_base + u * STREAM, STREAM), :] = out.T.astype(jnp.bfloat16)
            for i in range(seq // BQ):
                @pl.when(qi == i)
                def _():
                    for piece in range(i * BQ // half_len, (i + 1) * BQ // half_len):
                        @pl.when(home(piece)[0] == me)
                        def _():
                            o_keep(g, piece).start()

                        @pl.when(home(piece)[0] != me)
                        def _():
                            o_send(g, piece).start()
        for piece in range(n_pieces):
            @pl.when(home(piece)[0] == me)
            def _():
                o_keep(g, piece).wait()

    def wo_copy(g, nb, slot):
        rows = pl.ds(pl.multiple_of(g * depth, depth), depth)
        return pltpu.make_async_copy(wo_hbm.at[rows, pl.ds(pl.multiple_of(nb * OUT_COLS, OUT_COLS), OUT_COLS)], wo_scr.at[slot], wo_sem.at[slot])

    def y_copy(nb, slot):
        return pltpu.make_async_copy(ys_scr.at[slot], y_hbm.at[:, pl.ds(pl.multiple_of(nb * OUT_COLS, OUT_COLS), OUT_COLS)], ys_sem.at[slot])

    def combine(g):
        wo_copy(g, 0, 0).start()
        wo_copy(g, 1, 1).start()
        for src in range(n_cp):
            @pl.when(me != src)
            def _():
                for half in range(2):
                    o_recv(g, src, half).wait_recv()
        loads = [pltpu.make_async_copy(ogot_hbm.at[g, h], oc_scr.at[:, pl.ds(h * HEAD, HEAD)], oc_sem.at[h]) for h in range(n_cp)]
        for copy in loads:
            copy.start()
        for copy in loads:
            copy.wait()

        @pl.loop(0, n_out)
        def _(nb):
            slot = lax.rem(nb, 2)
            cols = pl.ds(pl.multiple_of(nb * OUT_COLS, OUT_COLS), OUT_COLS)
            wo_copy(g, nb, slot).wait()
            for rows in row_parts:
                y_scr[rows, cols] += jnp.dot(oc_scr[rows, :], wo_scr[slot], preferred_element_type=jnp.float32)

            @pl.when(nb + 2 < n_out)
            def _():
                wo_copy(g, nb + 2, slot).start()

            @pl.when(g == n_chunk - 1)
            def _():
                @pl.when(nb >= 2)
                def _():
                    y_copy(nb - 2, slot).wait()
                ys_scr[slot] = y_scr[:, cols].astype(jnp.bfloat16)
                y_copy(nb, slot).start()

    pl.loop(0, n_chunk)(project)
    pl.loop(0, n_chunk)(attend)
    pl.loop(0, n_chunk)(combine)

    for nb in range(n_out - 2, n_out):
        y_copy(nb, nb % 2).wait()

    @pl.loop(0, n_chunk)
    def _(g):
        o_sent(g)
        for dest in range(n_cp):
            @pl.when(me != dest)
            def _():
                to_peer(g, dest).wait_send()


def layer(x_loc, w_q, w_k, w_v, w_o, cos, sin, n_cp):
    n_loc, d_model = x_loc.shape
    width = w_q.shape[1]
    n_chunk = width // HEAD // n_cp
    seq = n_loc * n_cp
    bf16, f32 = jnp.bfloat16, jnp.float32
    shape = jax.ShapeDtypeStruct
    hbm = pl.BlockSpec(memory_space=pltpu.HBM)
    vmem = pl.BlockSpec(memory_space=pltpu.VMEM)
    dma = pltpu.SemaphoreType.DMA
    rows = pltpu.VMEM((seq, HEAD), bf16)
    stats = pltpu.VMEM((8, BQ), f32)
    score = pltpu.VMEM((BK, BQ), f32)
    pieces = shape((n_chunk, n_cp, 3, n_loc, HEAD), bf16)
    y, k_plain, v_plain, *_ = pl.pallas_call(
        functools.partial(layer_kernel, n_cp, n_chunk),
        in_specs=[hbm] * 5 + [vmem] * 2,
        out_specs=[hbm] * 6,
        out_shape=[shape((n_loc, w_o.shape[1]), bf16), shape((n_loc, width), bf16), shape((n_loc, width), bf16),
                   pieces, pieces, shape((n_chunk, n_cp, n_loc, HEAD), bf16)],
        scratch_shapes=[
            pltpu.VMEM((n_loc, d_model), bf16), pltpu.VMEM((3, d_model, LANES), bf16), pltpu.VMEM((2, 2, 3, n_loc, HEAD), bf16),
            rows, rows, rows, pltpu.VMEM((HEAD, seq), bf16), pltpu.VMEM((n_chunk, seq, HEAD), bf16), pltpu.VMEM((HEAD, BQ), f32),
            stats, stats, score, score,
            pltpu.VMEM((n_loc, n_cp * HEAD), bf16), pltpu.VMEM((2, n_cp * HEAD, OUT_COLS), bf16), pltpu.VMEM((n_loc, w_o.shape[1]), f32),
            pltpu.VMEM((2, n_loc, OUT_COLS), bf16),
            dma, dma((3,)), dma((2, 2, 3)), dma((n_chunk, n_cp)), dma((n_chunk, n_cp)), dma((2 * n_cp, 3)), dma((2,)),
            dma((n_chunk, 2 * n_cp)), dma((n_chunk, n_cp, 2)), dma((n_cp,)), dma((2,)), dma((2,))],
        compiler_params=pltpu.CompilerParams(collective_id=0, has_side_effects=True, vmem_limit_bytes=67043328),
        name="layer",
    )(x_loc, w_q, w_k, w_v, w_o, cos, sin)
    return y, k_plain, v_plain


def split_heads_kernel(k_ref, v_ref, k_out, v_out):
    k_out[...] = k_ref[...].reshape(k_out.shape)
    v_out[...] = v_ref[...].reshape(v_out.shape)


def split_heads(k_plain, v_plain):
    n_loc, width = k_plain.shape
    flat = pl.BlockSpec((COPY_ROWS, width), lambda i: (i, 0))
    split = pl.BlockSpec((COPY_ROWS, width // HEAD, HEAD), lambda i: (i, 0, 0))
    out = jax.ShapeDtypeStruct((n_loc, width // HEAD, HEAD), k_plain.dtype)
    return pl.pallas_call(
        split_heads_kernel, grid=(n_loc // COPY_ROWS,), in_specs=[flat, flat], out_specs=[split, split], out_shape=[out, out],
        compiler_params=pltpu.CompilerParams(vmem_limit_bytes=40 << 20), name="split_heads",
    )(k_plain, v_plain)


def solution(mesh):
    n_cp = mesh.shape['cp']

    def per_device(x_loc, w_q, w_k, w_v, w_o):
        n_loc = x_loc.shape[0]
        cos, sin = rope_tables(local_positions(lax.axis_index('cp'), n_cp, n_loc // 2))
        y_loc, k_plain, v_plain = layer(x_loc, w_q, w_k, w_v, w_o, cos, sin, n_cp)
        return y_loc, *split_heads(k_plain, v_plain)

    row_spec = P(('dp', 'cp'), None)
    kv_spec = P(('dp', 'cp'), None, None)
    full_spec = P(None, None)
    return jax.shard_map(per_device, mesh=mesh, in_specs=(row_spec, full_spec, full_spec, full_spec, full_spec), out_specs=(row_spec, kv_spec, kv_spec), check_vma=False)
```
